32 devices in a mesh: ta: 2 (over x), ha: 4 (over y, core), wa: 4 (over z).
Axes of the slice: x: 2, y: 2, z: 4, core: 2. Of those that a mesh axis runs over, the one named last changes fastest.
Arguments:
- volume: bfloat16 [2, 128, 64, 128], P('ta', 'ha', 'wa'), may hold values from -6 to 6
- cotangent: bfloat16 [2, 128, 64, 128], P('ta', 'ha', 'wa'), may hold values from -6 to 6
- kernel_one: bfloat16 [3, 3, 3, 128, 128], replicated, may hold values from -0.109375 to 0.109375
- kernel_two: bfloat16 [3, 3, 3, 128, 128], replicated, may hold values from -0.109375 to 0.109375
Outputs:
- d_volume: bfloat16 [2, 128, 64, 128], P('ta', 'ha', 'wa')
- grad_one: float32 [3, 3, 3, 128, 128], replicated
- grad_two: float32 [3, 3, 3, 128, 128], replicated
The draws below stay inside these ranges and needn't reach their ends.
All inputs are finite; a program needn't handle non-finite values.
Results may differ from the reference program's by a relative error of at most 0.0049.
Values may be sent and summed in bfloat16 or wider, within the bound.
A program may use at most 64 MiB of HBM per device.

```python
import jax
import jax.numpy as jnp
from jax import lax

CHANNELS = 128
FRAMES = 2
HEIGHT = 128
WIDTH_ALL = 64


def steps_of(rng, dims, shards, smallest, high):
    gain, own = 1.0, jax.random.fold_in(rng, 6)
    for dim, blocks in shards:
        draws = jnp.exp(jax.random.uniform(jax.random.fold_in(own, dim), (blocks,), jnp.float32, smallest / len(shards), high / len(shards)))
        gain = gain * jnp.repeat(draws, dims[dim] // blocks).reshape([-1 if axis == dim else 1 for axis in range(len(dims))])
    return gain


def centred(own_key, extent, spread, reach, split=(), dtype=jnp.bfloat16):
    array = spread * jax.random.normal(own_key, extent, jnp.float32)
    if split:
        array = array * steps_of(own_key, extent, split, -0.22, 0.18)
    return jnp.clip(array, -reach, reach).astype(dtype)


def setup_inputs(seed: int = 0) -> dict:
    splits = jax.random.split(jax.random.key(seed), 5)
    volume = centred(splits[0], (FRAMES, HEIGHT, WIDTH_ALL, CHANNELS), 1.0, 6.0, ((0, 2), (1, 4), (2, 4)))
    cotangent = centred(splits[1], (FRAMES, HEIGHT, WIDTH_ALL, CHANNELS), 1.0, 6.0, ((0, 2), (1, 4), (2, 4)))
    kernel_one = centred(splits[2], (3, 3, 3, CHANNELS, CHANNELS), (27 * CHANNELS) ** -0.5, 0.109375)
    kernel_two = centred(splits[3], (3, 3, 3, CHANNELS, CHANNELS), (27 * CHANNELS) ** -0.5, 0.109375)
    return {"volume": volume, "cotangent": cotangent, "kernel_one": kernel_one, "kernel_two": kernel_two}


def flip_swap(kernel):
    return jnp.swapaxes(kernel[::-1, ::-1, ::-1], 3, 4)

def pad_field(field):
    return jnp.pad(field.astype(jnp.float32), ((1, 1), (1, 1), (1, 1), (0, 0)))

def conv_full(field, kernel):
    frames, height, width, chans = field.shape
    padded = pad_field(field)
    total = jnp.zeros((frames * height * width, chans), jnp.float32)
    for kt in range(3):
        for kh in range(3):
            for kw in range(3):
                piece = padded[kt:kt + frames, kh:kh + height, kw:kw + width].reshape(-1, chans)
                total = total + jnp.dot(piece, kernel[kt, kh, kw].astype(jnp.float32), precision=lax.Precision.HIGHEST)
    return total.reshape(frames, height, width, chans)

def kernel_grad(field, other):
    frames, height, width, chans = field.shape
    padded = pad_field(field)
    right = other.astype(jnp.float32).reshape(-1, chans)
    blocks = []
    for kt in range(3):
        for kh in range(3):
            for kw in range(3):
                piece = padded[kt:kt + frames, kh:kh + height, kw:kw + width].reshape(-1, chans)
                blocks.append(jnp.dot(piece.T, right, precision=lax.Precision.HIGHEST))
    return jnp.stack(blocks).reshape(3, 3, 3, chans, chans)

def reference(volume, cotangent, kernel_one, kernel_two):
    pre = conv_full(volume, kernel_one)
    sig = jax.nn.sigmoid(pre)
    hidden = (pre * sig).astype(jnp.bfloat16)
    d_hidden = conv_full(cotangent, flip_swap(kernel_two))
    d_pre = (d_hidden * sig * (1.0 + pre * (1.0 - sig))).astype(jnp.bfloat16)
    d_volume = conv_full(d_pre, flip_swap(kernel_one)).astype(jnp.bfloat16)
    scale = 1.0 / jnp.sqrt(jnp.float32(FRAMES * HEIGHT * WIDTH_ALL))
    grad_two = kernel_grad(hidden, cotangent) * scale
    grad_one = kernel_grad(volume, d_pre) * scale
    return (d_volume, grad_one, grad_two)
```

```python
import functools

import jax
import jax.numpy as jnp
from jax import lax
from jax.experimental import pallas as pl
from jax.experimental.pallas import tpu as pltpu
from jax.sharding import PartitionSpec as P

MESH = pl.DeviceIdType.MESH
TILE = 16


class Sizes:
    def __init__(self, mesh):
        self.nt, self.nh, self.nw = mesh.shape["ta"], mesh.shape["ha"], mesh.shape["wa"]
        self.cores = 2 if self.nh % 2 == 0 else 1
        self.rows = self.nh // self.cores
        self.plane = self.nt * self.rows
        self.devices = self.nt * self.nh * self.nw


def chunks_of(total, devices, pieces):
    units = -(-total // devices)
    pieces = min(pieces, units)
    cuts = [units * i // pieces for i in range(pieces + 1)]
    return [(a * devices, (b - a) * devices) for a, b in zip(cuts, cuts[1:])]


class Reduce:
    def __init__(self, sizes, where, source, out, first, tiles, base, bufs, send, recv, sem):
        self.s, self.source, self.out = sizes, source, out
        self.ti, self.hi, self.wi = where
        self.core = self.hi % sizes.cores
        self.half = tiles // sizes.cores
        self.part = self.half // sizes.plane
        self.shard = self.part // sizes.nw
        self.me = self.ti * sizes.rows + self.hi // sizes.cores
        self.first, self.base = first, base
        self.land_core, self.land_plane, self.land_wa, self.acc = bufs
        self.send, self.recv, self.sem = send, recv, sem
        self.open = []

    def copy(self, src, dst, device):
        made = pltpu.make_async_remote_copy(
            src_ref=src, dst_ref=dst, send_sem=self.send.at[self.sem], recv_sem=self.recv.at[self.sem],
            device_id=device, device_id_type=MESH,
        )
        self.sem += 1
        made.start()
        self.open.append(made)
        return made

    def core_device(self):
        return (self.ti, self.hi + 1 - 2 * self.core, self.wi)

    def plane_device(self, step):
        to = lax.rem(self.me + step, self.s.plane)
        return to, (to // self.s.rows, (to % self.s.rows) * self.s.cores + self.core, self.wi)

    def wa_device(self, step):
        to = lax.rem(self.wi + step, self.s.nw)
        return to, (self.ti, self.hi, to)

    def start_core(self):
        s = self.s
        self.waits = []
        if s.cores == 2:
            other = self.source.at[pl.ds(self.first + (1 - self.core) * self.half, self.half)]
            land = self.land_core.at[pl.ds(self.base // 2, self.half)]
            self.waits = [self.copy(other, land, self.core_device())]

    def start_plane(self):
        s = self.s
        for made in self.waits:
            made.wait_recv()
        mine = self.source[pl.ds(self.first + self.core * self.half, self.half)]
        at = self.base // s.cores
        if s.cores == 2:
            mine = mine.astype(jnp.float32) + self.land_core[pl.ds(at, self.half)].astype(jnp.float32)
        self.acc[pl.ds(at, self.half)] = mine.astype(jnp.bfloat16)
        self.waits = []
        for step in range(1, s.plane):
            to, device = self.plane_device(step)
            src = self.acc.at[pl.ds(at + to * self.part, self.part)]
            dst = self.land_plane.at[step - 1, pl.ds(at // s.plane, self.part)]
            self.waits.append(self.copy(src, dst, device))

    def start_wa(self):
        s = self.s
        for made in self.waits:
            made.wait_recv()
        at = self.base // s.cores
        low = at // s.plane
        total = self.acc[pl.ds(at + self.me * self.part, self.part)].astype(jnp.float32)
        for step in range(1, s.plane):
            total = total + self.land_plane[step - 1, pl.ds(low, self.part)].astype(jnp.float32)
        spare = self.land_plane.at[s.plane - 1]
        spare[pl.ds(low, self.part)] = total.astype(jnp.bfloat16)
        self.waits = []
        for step in range(1, s.nw):
            to, device = self.wa_device(step)
            src = spare.at[pl.ds(low + to * self.shard, self.shard)]
            dst = self.land_wa.at[step - 1, pl.ds(low // s.nw, self.shard)]
            self.waits.append(self.copy(src, dst, device))

    def back_wa(self):
        s = self.s
        for made in self.waits:
            made.wait_recv()
        low = self.base // s.cores // s.plane
        spare = self.land_plane.at[s.plane - 1]
        total = spare[pl.ds(low + self.wi * self.shard, self.shard)].astype(jnp.float32)
        for step in range(1, s.nw):
            total = total + self.land_wa[step - 1, pl.ds(low // s.nw, self.shard)].astype(jnp.float32)
        here = self.first + self.core * self.half + self.me * self.part
        mine = self.out.at[pl.ds(here + self.wi * self.shard, self.shard)]
        mine[...] = total.astype(jnp.bfloat16)
        self.waits = [self.copy(mine, mine, self.wa_device(step)[1]) for step in range(1, s.nw)]

    def back_plane(self):
        s = self.s
        for made in self.waits:
            made.wait_recv()
        here = self.first + self.core * self.half + self.me * self.part
        mine = self.out.at[pl.ds(here, self.part)]
        self.waits = [self.copy(mine, mine, self.plane_device(step)[1]) for step in range(1, s.plane)]

    def back_core(self):
        for made in self.waits:
            made.wait_recv()
        self.waits = []
        if self.s.cores == 2:
            mine = self.out.at[pl.ds(self.first + self.core * self.half, self.half)]
            self.waits = [self.copy(mine, mine, self.core_device())]

    def finish(self):
        for made in self.waits:
            made.wait_recv()
        for made in self.open:
            made.wait_send()


def copies_of(sizes):
    return 2 * ((sizes.cores - 1) + (sizes.plane - 1) + (sizes.nw - 1))


STAGES = ("start_core", "start_plane", "start_wa", "back_wa", "back_plane", "back_core", "finish")


def reduce_scratch(sizes, tiles, count):
    half = tiles // sizes.cores
    part = half // sizes.plane
    return [
        pltpu.VMEM((half, TILE, 128), jnp.bfloat16),
        pltpu.VMEM((sizes.plane, part, TILE, 128), jnp.bfloat16),
        pltpu.VMEM((max(sizes.nw - 1, 1), part // sizes.nw, TILE, 128), jnp.bfloat16),
        pltpu.VMEM((half, TILE, 128), jnp.bfloat16),
        pltpu.SemaphoreType.DMA((count * copies_of(sizes),)),
        pltpu.SemaphoreType.DMA((count * copies_of(sizes),)),
    ]


def reduce_partners(sizes, where):
    ti, hi, wi = where
    core = hi % sizes.cores
    me = ti * sizes.rows + hi // sizes.cores
    found = []
    if sizes.cores == 2:
        found.append((ti, hi + 1 - 2 * core, wi))
    for step in range(1, sizes.plane):
        to = lax.rem(me + step, sizes.plane)
        found.append((to // sizes.rows, (to % sizes.rows) * sizes.cores + core, wi))
    for step in range(1, sizes.nw):
        found.append((ti, hi, lax.rem(wi + step, sizes.nw)))
    return found


def reduce_kernel(sizes, ranges, part_ref, out_ref, *scratch):
    bufs, (send, recv) = scratch[:4], scratch[4:]
    where = (lax.axis_index("ta"), lax.axis_index("ha"), lax.axis_index("wa"))
    partners = reduce_partners(sizes, where)
    barrier = pltpu.get_barrier_semaphore()
    for device in partners:
        pl.semaphore_signal(barrier, inc=1, device_id=device, device_id_type=MESH)
    pl.semaphore_wait(barrier, len(partners))
    runs = [
        Reduce(sizes, where, part_ref, out_ref, first, tiles, first, bufs, send, recv, i * copies_of(sizes))
        for i, (first, tiles) in enumerate(ranges)
    ]
    for stage in STAGES:
        for run in runs:
            getattr(run, stage)()


def all_sum(sizes, parts, pieces):
    total = parts.shape[0]
    ranges = chunks_of(total, sizes.devices, pieces)
    tiles = sum(size for _, size in ranges)
    parts = jnp.pad(parts, ((0, tiles - total), (0, 0), (0, 0)))
    return pl.pallas_call(
        functools.partial(reduce_kernel, sizes, ranges),
        out_shape=jax.ShapeDtypeStruct((tiles, TILE, 128), jnp.bfloat16),
        in_specs=[pl.BlockSpec(memory_space=pltpu.VMEM)],
        out_specs=pl.BlockSpec(memory_space=pltpu.VMEM),
        scratch_shapes=reduce_scratch(sizes, tiles, len(ranges)),
        compiler_params=pltpu.CompilerParams(
            collective_id=0, has_side_effects=True, vmem_limit_bytes=48 * 1024 * 1024
        ),
    )(parts)[:total]


def padded_2(cells, sides, width):
    for axis, dim in sides:
        count = lax.axis_size(axis)
        ends = count - 1
        head = lax.slice_in_dim(cells, 0, width, axis=dim)
        tail = lax.slice_in_dim(cells, cells.shape[dim] - width, cells.shape[dim], axis=dim)
        cells = jnp.concatenate(
            [
                lax.ppermute(tail, axis, [(i, (i + 1) % count) for i in range(ends)]),
                cells,
                lax.ppermute(head, axis, [((i + 1) % count, i) for i in range(ends)]),
            ],
            axis=dim,
        )
    return cells


def flip_swap(kernel):
    return jnp.swapaxes(kernel[::-1, ::-1, ::-1], 3, 4)


def window_rows(padded, offset_t, offset_h):
    frames = padded.shape[0] - 2
    height = padded.shape[1] - 2
    width = padded.shape[2] - 2
    chans = padded.shape[3]
    pieces = [
        padded[offset_t : offset_t + frames, offset_h : offset_h + height, shift : shift + width]
        for shift in range(3)
    ]
    return jnp.concatenate(pieces, axis=-1).reshape(-1, 3 * chans)


def conv_local(padded, kernel):
    frames = padded.shape[0] - 2
    height = padded.shape[1] - 2
    width = padded.shape[2] - 2
    chans = padded.shape[3]
    total = jnp.zeros((frames * height * width, chans), jnp.float32)
    for offset_t in range(3):
        for offset_h in range(3):
            rows = window_rows(padded, offset_t, offset_h)
            total = total + jnp.dot(
                rows,
                kernel[offset_t, offset_h].reshape(3 * chans, chans),
                preferred_element_type=jnp.float32,
            )
    return total.reshape(frames, height, width, chans)


def kernel_local(padded, other):
    chans = padded.shape[3]
    right = other.reshape(-1, chans)
    blocks = []
    for offset_t in range(3):
        for offset_h in range(3):
            rows = window_rows(padded, offset_t, offset_h)
            product = lax.dot_general(
                rows, right, (((0,), (0,)), ((), ())), preferred_element_type=jnp.float32
            )
            blocks.append(product.reshape(3, chans, chans))
    return jnp.stack(blocks).reshape(3, 3, 3, chans, chans)


def body(sizes, volume, cotangent, kernel_one, kernel_two):
    stacked = jnp.stack((volume, cotangent))
    padded_both = padded_2(stacked, (("ta", 1), ("ha", 2), ("wa", 3)), 1)
    volume_pad = padded_both[0]
    cotangent_pad = padded_both[1]
    pre = conv_local(volume_pad, kernel_one)
    sig = jax.nn.sigmoid(pre)
    hidden = (pre * sig).astype(jnp.bfloat16)
    d_hidden = conv_local(cotangent_pad, flip_swap(kernel_two))
    d_pre = (d_hidden * sig * (1.0 + pre * (1.0 - sig))).astype(jnp.bfloat16)
    total_cells = (
        volume.shape[0]
        * volume.shape[1]
        * volume.shape[2]
        * lax.axis_size("ta")
        * lax.axis_size("ha")
        * lax.axis_size("wa")
    )
    scale = 1.0 / jnp.sqrt(jnp.float32(total_cells))
    part_two = flip_swap(kernel_local(cotangent_pad, hidden))
    d_pre_pad = padded_2(d_pre, (("ta", 0), ("ha", 1), ("wa", 2)), 1)
    d_volume = conv_local(d_pre_pad, flip_swap(kernel_one)).astype(jnp.bfloat16)
    part_one = kernel_local(volume_pad, d_pre)
    both = jnp.concatenate([part_one.reshape(-1), part_two.reshape(-1)]).astype(jnp.bfloat16)
    summed = all_sum(sizes, both.reshape(-1, TILE, 128), 4).reshape((2,) + kernel_one.shape)
    summed = summed.astype(jnp.float32) * scale
    return (d_volume, summed[0], summed[1])


def solution(mesh):
    in_specs = (P("ta", "ha", "wa", None), P("ta", "ha", "wa", None), P(), P())
    out_specs = (P("ta", "ha", "wa", None), P(), P())
    return jax.shard_map(
        functools.partial(body, Sizes(mesh)), mesh=mesh, in_specs=in_specs, out_specs=out_specs, check_vma=False)
```

```python
import functools

import jax
import jax.numpy as jnp
from jax import lax
from jax.experimental import pallas as pl
from jax.experimental.pallas import tpu as pltpu
from jax.sharding import PartitionSpec as P

MESH = pl.DeviceIdType.MESH
TILE = 16


class Sizes:
    def __init__(self, mesh):
        self.nt, self.nh, self.nw = mesh.shape["ta"], mesh.shape["ha"], mesh.shape["wa"]
        self.cores = 2 if self.nh % 2 == 0 else 1
        self.rows = self.nh // self.cores
        self.plane = self.nt * self.rows
        self.devices = self.nt * self.nh * self.nw


def chunks_of(total, devices, pieces):
    units = -(-total // devices)
    pieces = min(pieces, units)
    cuts = [units * i // pieces for i in range(pieces + 1)]
    return [(a * devices, (b - a) * devices) for a, b in zip(cuts, cuts[1:])]


class Reduce:
    def __init__(self, sizes, where, source, out, first, tiles, base, bufs, send, recv, sem):
        self.s, self.source, self.out = sizes, source, out
        self.ti, self.hi, self.wi = where
        self.core = self.hi % sizes.cores
        self.half = tiles // sizes.cores
        self.part = self.half // sizes.plane
        self.shard = self.part // sizes.nw
        self.me = self.ti * sizes.rows + self.hi // sizes.cores
        self.first, self.base = first, base
        self.land_core, self.land_plane, self.land_wa, self.acc = bufs
        self.send, self.recv, self.sem = send, recv, sem
        self.open = []

    def copy(self, src, dst, device):
        made = pltpu.make_async_remote_copy(
            src_ref=src, dst_ref=dst, send_sem=self.send.at[self.sem], recv_sem=self.recv.at[self.sem],
            device_id=device, device_id_type=MESH,
        )
        self.sem += 1
        made.start()
        self.open.append(made)
        return made

    def core_device(self):
        return (self.ti, self.hi + 1 - 2 * self.core, self.wi)

    def plane_device(self, step):
        to = lax.rem(self.me + step, self.s.plane)
        return to, (to // self.s.rows, (to % self.s.rows) * self.s.cores + self.core, self.wi)

    def wa_device(self, step):
        to = lax.rem(self.wi + step, self.s.nw)
        return to, (self.ti, self.hi, to)

    def start_core(self):
        s = self.s
        self.waits = []
        if s.cores == 2:
            other = self.source.at[pl.ds(self.first + (1 - self.core) * self.half, self.half)]
            land = self.land_core.at[pl.ds(self.base // 2, self.half)]
            self.waits = [self.copy(other, land, self.core_device())]

    def start_plane(self):
        s = self.s
        for made in self.waits:
            made.wait_recv()
        mine = self.source[pl.ds(self.first + self.core * self.half, self.half)]
        at = self.base // s.cores
        if s.cores == 2:
            mine = mine.astype(jnp.float32) + self.land_core[pl.ds(at, self.half)].astype(jnp.float32)
        self.acc[pl.ds(at, self.half)] = mine.astype(jnp.bfloat16)
        self.waits = []
        for step in range(1, s.plane):
            to, device = self.plane_device(step)
            src = self.acc.at[pl.ds(at + to * self.part, self.part)]
            dst = self.land_plane.at[step - 1, pl.ds(at // s.plane, self.part)]
            self.waits.append(self.copy(src, dst, device))

    def start_wa(self):
        s = self.s
        for made in self.waits:
            made.wait_recv()
        at = self.base // s.cores
        low = at // s.plane
        total = self.acc[pl.ds(at + self.me * self.part, self.part)].astype(jnp.float32)
        for step in range(1, s.plane):
            total = total + self.land_plane[step - 1, pl.ds(low, self.part)].astype(jnp.float32)
        spare = self.land_plane.at[s.plane - 1]
        spare[pl.ds(low, self.part)] = total.astype(jnp.bfloat16)
        self.waits = []
        for step in range(1, s.nw):
            to, device = self.wa_device(step)
            src = spare.at[pl.ds(low + to * self.shard, self.shard)]
            dst = self.land_wa.at[step - 1, pl.ds(low // s.nw, self.shard)]
            self.waits.append(self.copy(src, dst, device))

    def back_wa(self):
        s = self.s
        for made in self.waits:
            made.wait_recv()
        low = self.base // s.cores // s.plane
        spare = self.land_plane.at[s.plane - 1]
        total = spare[pl.ds(low + self.wi * self.shard, self.shard)].astype(jnp.float32)
        for step in range(1, s.nw):
            total = total + self.land_wa[step - 1, pl.ds(low // s.nw, self.shard)].astype(jnp.float32)
        here = self.first + self.core * self.half + self.me * self.part
        mine = self.out.at[pl.ds(here + self.wi * self.shard, self.shard)]
        mine[...] = total.astype(jnp.bfloat16)
        self.waits = [self.copy(mine, mine, self.wa_device(step)[1]) for step in range(1, s.nw)]

    def back_plane(self):
        s = self.s
        for made in self.waits:
            made.wait_recv()
        here = self.first + self.core * self.half + self.me * self.part
        mine = self.out.at[pl.ds(here, self.part)]
        self.waits = [self.copy(mine, mine, self.plane_device(step)[1]) for step in range(1, s.plane)]

    def back_core(self):
        for made in self.waits:
            made.wait_recv()
        self.waits = []
        if self.s.cores == 2:
            mine = self.out.at[pl.ds(self.first + self.core * self.half, self.half)]
            self.waits = [self.copy(mine, mine, self.core_device())]

    def finish(self):
        for made in self.waits:
            made.wait_recv()
        for made in self.open:
            made.wait_send()


def copies_of(sizes):
    return 2 * ((sizes.cores - 1) + (sizes.plane - 1) + (sizes.nw - 1))


STAGES = ("start_core", "start_plane", "start_wa", "back_wa", "back_plane", "back_core", "finish")


def reduce_scratch(sizes, tiles, count):
    half = tiles // sizes.cores
    part = half // sizes.plane
    return [
        pltpu.VMEM((half, TILE, 128), jnp.bfloat16),
        pltpu.VMEM((sizes.plane, part, TILE, 128), jnp.bfloat16),
        pltpu.VMEM((max(sizes.nw - 1, 1), part // sizes.nw, TILE, 128), jnp.bfloat16),
        pltpu.VMEM((half, TILE, 128), jnp.bfloat16),
        pltpu.SemaphoreType.DMA((count * copies_of(sizes),)),
        pltpu.SemaphoreType.DMA((count * copies_of(sizes),)),
    ]


def reduce_partners(sizes, where):
    ti, hi, wi = where
    core = hi % sizes.cores
    me = ti * sizes.rows + hi // sizes.cores
    found = []
    if sizes.cores == 2:
        found.append((ti, hi + 1 - 2 * core, wi))
    for step in range(1, sizes.plane):
        to = lax.rem(me + step, sizes.plane)
        found.append((to // sizes.rows, (to % sizes.rows) * sizes.cores + core, wi))
    for step in range(1, sizes.nw):
        found.append((ti, hi, lax.rem(wi + step, sizes.nw)))
    return found


DIRS = [(dt, dh) for dt in (-1, 0, 1) for dh in (-1, 0, 1) if (dt, dh) != (0, 0)]


class Halo:
    def __init__(self, sizes, where, sources, landings, send, recv):
        self.s, self.where = sizes, where
        self.sources, self.landings = sources, landings
        self.frames, self.height = sources[0].shape[0], sources[0].shape[1]
        self.send, self.recv = send, recv

    def exists(self, dt, dh):
        ti, hi = self.where[0] + dt, self.where[1] + dh
        return (ti >= 0) & (ti < self.s.nt) & (hi >= 0) & (hi < self.s.nh)

    def made(self, field, dt, dh):
        def span(step, extent):
            first = {-1: 0, 0: 0, 1: extent - 1}[step]
            land = {-1: extent + 1, 0: 1, 1: 0}[step]
            return first, land, extent if step == 0 else 1

        t0, t1, tn = span(dt, self.frames)
        h0, h1, hn = span(dh, self.height)
        slot = field * len(DIRS) + DIRS.index((dt, dh))
        return pltpu.make_async_remote_copy(
            src_ref=self.sources[field].at[pl.ds(t0, tn), pl.ds(h0, hn)],
            dst_ref=self.landings[field].at[pl.ds(t1, tn), pl.ds(h1, hn)],
            send_sem=self.send.at[slot],
            recv_sem=self.recv.at[slot],
            device_id=(self.where[0] + dt, self.where[1] + dh, self.where[2]),
            device_id_type=MESH,
        )

    def start(self):
        for dt, dh in DIRS:

            @pl.when(self.exists(dt, dh))
            def _():
                for field in range(len(self.sources)):
                    self.made(field, dt, dh).start()

    def zero(self):
        def span(step, extent):
            return {-1: (0, 1), 0: (1, extent), 1: (extent + 1, 1)}[step]

        for dt, dh in DIRS:

            @pl.when(jnp.logical_not(self.exists(dt, dh)))
            def _():
                for landing in self.landings:
                    part = landing.at[pl.ds(*span(dt, self.frames)), pl.ds(*span(dh, self.height))]
                    part[...] = jnp.zeros(part.shape, part.dtype)

    def wait_recv(self):
        for dt, dh in DIRS:

            @pl.when(self.exists(-dt, -dh))
            def _():
                for field in range(len(self.sources)):
                    self.made(field, dt, dh).wait_recv()

    def wait_send(self):
        for dt, dh in DIRS:

            @pl.when(self.exists(dt, dh))
            def _():
                for field in range(len(self.sources)):
                    self.made(field, dt, dh).wait_send()


class Columns:
    def __init__(self, sizes, where, landings, lines, shifted, edge_out, edge_in, wide, send, recv):
        self.s, self.where, self.landings, self.lines = sizes, where, landings, lines
        self.shifted, self.out, self.into, self.wide = shifted, edge_out, edge_in, wide
        self.send, self.recv = send, recv
        self.count = landings[0].shape[0] * landings[0].shape[1]
        self.width = landings[0].shape[2]

    def exists(self, side):
        to = self.where[2] + (1 if side else -1)
        return (to >= 0) & (to < self.s.nw)

    def made(self, side):
        return pltpu.make_async_remote_copy(
            src_ref=self.out.at[side],
            dst_ref=self.into.at[1 - side],
            send_sem=self.send.at[side],
            recv_sem=self.recv.at[1 - side],
            device_id=(self.where[0], self.where[1], self.where[2] + (1 if side else -1)),
            device_id_type=MESH,
        )

    def start(self):
        cells = self.count * self.width
        for field, landing in enumerate(self.landings):
            line = self.lines[field]
            line[pl.ds(8, cells), :] = landing[...].astype(jnp.float32).reshape(cells, 128)
            for side in range(2):
                edge = line[pl.ds(8 + side * (self.width - 1), self.count, stride=self.width), :]
                self.out[side, field] = edge.astype(jnp.bfloat16)
        for side in range(2):
            pl.when(self.exists(side))(lambda side=side: self.made(side).start())
            zero = jnp.zeros(self.into.shape[1:], jnp.bfloat16)

            @pl.when(jnp.logical_not(self.exists(side)))
            def _():
                self.into[side] = zero

        frames = self.landings[0].shape[0]
        for field, landing in enumerate(self.landings):
            self.wide[field, :, :, 128:256] = landing[...].reshape(frames, -1, 128)

    def finish(self):
        for side in range(2):
            pl.when(self.exists(side))(lambda side=side: self.made(1 - side).wait_recv())
        cells = self.count * self.width
        frames = self.landings[0].shape[0]
        for field in range(len(self.landings)):
            for side in range(2):
                line = self.lines[field]
                self.shifted[...] = line[pl.ds(7 + 2 * side, cells), :]
                at = side * (self.width - 1)
                edge = self.into[side, field].astype(jnp.float32)
                self.shifted[pl.ds(at, self.count, stride=self.width), :] = edge
                moved = self.shifted[...].astype(jnp.bfloat16).reshape(frames, -1, 128)
                self.wide[field, :, :, 256 * side : 256 * side + 128] = moved

    def wait_send(self):
        for side in range(2):
            pl.when(self.exists(side))(lambda side=side: self.made(side).wait_send())


def conv_rows(wide, field, frame, first, rows, width, weights):
    total = None
    for tap in range(9):
        at = (tap % 3) * width + first
        piece = wide[field, frame + tap // 3, pl.ds(at, rows), :]
        product = jnp.dot(piece, weights[tap], preferred_element_type=jnp.float32)
        total = product if total is None else total + product
    return total


def kernel(
    sizes, ranges, volume, cotangent, one, two, d_volume, sums,
    fields, d_fields, lines, shifted, edge_out, edge_in, d_out, d_in, wide, d_wide,
    flip_one, flip_two, d_pre, part, turned, halo_send, halo_recv, col_send, col_recv, *scratch,
):
    bufs, (send, recv) = scratch[:4], scratch[4:]
    where = (lax.axis_index("ta"), lax.axis_index("ha"), lax.axis_index("wa"))
    frames, height, width, _ = volume.shape
    cells = height * width
    block = 256 if cells % 256 == 0 else cells
    partners = reduce_partners(sizes, where)
    halo = Halo(
        sizes, where, [volume, cotangent], [fields.at[0], fields.at[1]], halo_send.at[0], halo_recv.at[0]
    )
    d_halo = Halo(sizes, where, [d_pre], [d_fields], halo_send.at[1], halo_recv.at[1])
    barrier = pltpu.get_barrier_semaphore()
    for device in partners:
        pl.semaphore_signal(barrier, inc=1, device_id=device, device_id_type=MESH)
    for dt, dh in DIRS:

        @pl.when(halo.exists(dt, dh))
        def _():
            device = (where[0] + dt, where[1] + dh, where[2])
            pl.semaphore_signal(barrier, inc=1, device_id=device, device_id_type=MESH)

    near = sum(halo.exists(dt, dh).astype(jnp.int32) for dt, dh in DIRS)
    pl.semaphore_wait(barrier, len(partners) + near)
    halo.start()
    halo.zero()
    d_halo.zero()
    inner = (pl.ds(1, frames), pl.ds(1, height))
    for field, ref in enumerate((volume, cotangent)):
        fields.at[field].at[inner][...] = ref[...]
    for source, flipped in ((two, flip_two), (one, flip_one)):
        for tap in range(9):
            for kw in range(3):
                square = source[8 - tap, pl.ds((2 - kw) * 128, 128), :].astype(jnp.float32)
                flipped[tap, pl.ds(kw * 128, 128), :] = square.T.astype(jnp.bfloat16)
    halo.wait_recv()
    columns = Columns(
        sizes, where, [fields.at[0], fields.at[1]], [lines.at[0], lines.at[1]], shifted,
        edge_out, edge_in, wide, col_send.at[0], col_recv.at[0],
    )
    columns.start()
    columns.finish()
    for frame in range(frames):
        for first in range(0, cells, block):
            pre = conv_rows(wide, 0, frame, first, block, width, one)
            d_hidden = conv_rows(wide, 1, frame, first, block, width, flip_two)
            sig = 1.0 / (1.0 + jnp.exp(-pre))
            hidden = pre * sig
            grad = d_hidden * sig * (1.0 + pre * (1.0 - sig))
            at = pl.ds(frame * cells + first, block)
            turned[0, :, at] = hidden.T.astype(jnp.bfloat16)
            turned[1, :, at] = grad.T.astype(jnp.bfloat16)
            rounded = grad.astype(jnp.bfloat16).reshape(1, block // width, width, 128)
            d_pre[pl.ds(frame, 1), pl.ds(first // width, block // width)] = rounded
    d_halo.start()
    d_fields.at[inner][...] = d_pre[...]
    middle = part.shape[0] // 2
    real = 27 * 128 // TILE
    for base in (0, middle):
        if middle > real:
            part[pl.ds(base + real, middle - real)] = jnp.zeros((middle - real, TILE, 128), jnp.bfloat16)

    def gradient(field, side, tap):
        total = None
        for frame in range(frames):
            piece = wide[field, frame + tap // 3, pl.ds((tap % 3) * width, cells), :]
            left = turned[side, :, pl.ds(frame * cells, cells)]
            product = jnp.dot(left, piece, preferred_element_type=jnp.float32)
            total = product if total is None else total + product
        return total

    for tap in range(9):
        product = gradient(1, 0, tap).astype(jnp.bfloat16)
        for kw in range(3):
            at = ((8 - tap) * 3 + 2 - kw) * (128 // TILE)
            square = product[:, kw * 128 : kw * 128 + 128]
            part[pl.ds(at, 128 // TILE)] = square.reshape(128 // TILE, TILE, 128)
    runs = [
        Reduce(sizes, where, part, sums, first, tiles, first, bufs, send, recv, i * copies_of(sizes))
        for i, (first, tiles) in enumerate(ranges)
    ]
    early, late = runs[: len(runs) // 2], runs[len(runs) // 2 :]
    for run in early:
        run.start_core()
    for tap in range(9):
        product = gradient(0, 1, tap)
        for kw in range(3):
            at = middle + (tap * 3 + kw) * (128 // TILE)
            square = product[:, kw * 128 : kw * 128 + 128].T.astype(jnp.bfloat16)
            part[pl.ds(at, 128 // TILE)] = square.reshape(128 // TILE, TILE, 128)
    for run in late:
        run.start_core()
    for run in early:
        run.start_plane()
    d_halo.wait_recv()
    d_columns = Columns(
        sizes, where, [d_fields], [lines.at[0]], shifted, d_out, d_in, d_wide, col_send.at[1], col_recv.at[1]
    )
    d_columns.start()
    for run in late:
        run.start_plane()
    d_columns.finish()
    for frame in range(frames):
        for first in range(0, cells, block):
            total = conv_rows(d_wide, 0, frame, first, block, width, flip_one)
            total = total.astype(jnp.bfloat16).reshape(1, block // width, width, 128)
            d_volume[pl.ds(frame, 1), pl.ds(first // width, block // width)] = total
    for stage in STAGES[2:]:
        for run in runs:
            getattr(run, stage)()
    halo.wait_send()
    d_halo.wait_send()
    columns.wait_send()
    d_columns.wait_send()


def body(sizes, volume, cotangent, kernel_one, kernel_two):
    frames, height, width, chans = volume.shape
    real = 27 * chans // TILE
    ranges = chunks_of(real, sizes.devices, 2)
    middle = sum(tiles for _, tiles in ranges)
    ranges = ranges + [(middle + first, tiles) for first, tiles in ranges]
    tiles = 2 * middle
    tall, high = frames + 2, height + 2
    count = tall * high
    half = jnp.bfloat16
    vmem = pl.BlockSpec(memory_space=pltpu.VMEM)
    d_volume, sums = pl.pallas_call(
        functools.partial(kernel, sizes, ranges),
        out_shape=(
            jax.ShapeDtypeStruct(volume.shape, half),
            jax.ShapeDtypeStruct((tiles, TILE, chans), half),
        ),
        in_specs=[vmem] * 4,
        out_specs=(vmem, vmem),
        scratch_shapes=[
            pltpu.VMEM((2, tall, high, width, chans), half),
            pltpu.VMEM((tall, high, width, chans), half),
            pltpu.VMEM((2, count * width + 16, chans), jnp.float32),
            pltpu.VMEM((count * width, chans), jnp.float32),
            pltpu.VMEM((2, 2, count, chans), half),
            pltpu.VMEM((2, 2, count, chans), half),
            pltpu.VMEM((2, 1, count, chans), half),
            pltpu.VMEM((2, 1, count, chans), half),
            pltpu.VMEM((2, tall, high * width, 3 * chans), half),
            pltpu.VMEM((1, tall, high * width, 3 * chans), half),
            pltpu.VMEM((9, 3 * chans, chans), half),
            pltpu.VMEM((9, 3 * chans, chans), half),
            pltpu.VMEM(volume.shape, half),
            pltpu.VMEM((tiles, TILE, chans), half),
            pltpu.VMEM((2, chans, frames * height * width), half),
            pltpu.SemaphoreType.DMA((2, 2 * len(DIRS))),
            pltpu.SemaphoreType.DMA((2, 2 * len(DIRS))),
            pltpu.SemaphoreType.DMA((2, 2)),
            pltpu.SemaphoreType.DMA((2, 2)),
        ]
        + reduce_scratch(sizes, tiles, len(ranges)),
        compiler_params=pltpu.CompilerParams(
            collective_id=0, has_side_effects=True, vmem_limit_bytes=56 * 1024 * 1024
        ),
    )(volume, cotangent, kernel_one.reshape(9, 3 * chans, chans), kernel_two.reshape(9, 3 * chans, chans))
    scale = 1.0 / jnp.sqrt(jnp.float32(frames * height * width * sizes.devices))

    def scaled(first):
        return sums[first : first + real].reshape(kernel_one.shape).astype(jnp.float32) * scale

    return d_volume, scaled(middle), scaled(0)


def solution(mesh):
    in_specs = (P("ta", "ha", "wa", None), P("ta", "ha", "wa", None), P(), P())
    out_specs = (P("ta", "ha", "wa", None), P(), P())
    return jax.shard_map(
        functools.partial(body, Sizes(mesh)),
        mesh=mesh, in_specs=in_specs, out_specs=out_specs, check_vma=False,
    )
```

```python
import functools

import jax
import jax.numpy as jnp
from jax import lax
from jax.experimental import pallas as pl
from jax.experimental.pallas import tpu as pltpu
from jax.sharding import PartitionSpec as P

MESH = pl.DeviceIdType.MESH
TILE = 16


class Sizes:
    def __init__(self, mesh):
        self.nt, self.nh, self.nw = mesh.shape["ta"], mesh.shape["ha"], mesh.shape["wa"]
        self.cores = 2 if self.nh % 2 == 0 else 1
        self.rows = self.nh // self.cores
        self.plane = self.nt * self.rows
        self.devices = self.nt * self.nh * self.nw


def chunks_of(total, devices, pieces):
    units = -(-total // devices)
    pieces = min(pieces, units)
    cuts = [units * i // pieces for i in range(pieces + 1)]
    return [(a * devices, (b - a) * devices) for a, b in zip(cuts, cuts[1:])]


class Reduce:
    def __init__(self, sizes, where, source, out, first, tiles, base, bufs, send, recv, sem):
        self.s, self.source, self.out = sizes, source, out
        self.ti, self.hi, self.wi = where
        self.core = self.hi % sizes.cores
        self.tiles = tiles
        self.half = tiles // sizes.cores
        self.part = self.half // sizes.plane
        self.shard = self.part // sizes.nw
        self.me = self.ti * sizes.rows + self.hi // sizes.cores
        self.first, self.base = first, base
        self.land_core, self.land_plane, self.land_wa, self.acc = bufs
        self.send, self.recv, self.sem = send, recv, sem
        self.open = []

    def copy(self, src, dst, device):
        made = pltpu.make_async_remote_copy(
            src_ref=src, dst_ref=dst, send_sem=self.send.at[self.sem], recv_sem=self.recv.at[self.sem],
            device_id=device, device_id_type=MESH,
        )
        self.sem += 1
        made.start()
        self.open.append(made)
        return made

    def core_device(self):
        return (self.ti, self.hi + 1 - 2 * self.core, self.wi)

    def plane_device(self, step):
        to = lax.rem(self.me + step, self.s.plane)
        return to, (to // self.s.rows, (to % self.s.rows) * self.s.cores + self.core, self.wi)

    def wa_device(self, step):
        to = lax.rem(self.wi + step, self.s.nw)
        return to, (self.ti, self.hi, to)

    def start_core(self):
        s = self.s
        self.waits = []
        if s.cores == 2:
            other = self.source.at[pl.ds(self.first + (1 - self.core) * self.half, self.half)]
            land = self.land_core.at[pl.ds(self.base // 2, self.half)]
            self.waits = [self.copy(other, land, self.core_device())]

    def start_plane(self):
        s = self.s
        for made in self.waits:
            made.wait_recv()
        mine = self.source[pl.ds(self.first + self.core * self.half, self.half)]
        at = self.base // s.cores
        if s.cores == 2:
            mine = mine.astype(jnp.float32) + self.land_core[pl.ds(at, self.half)].astype(jnp.float32)
        self.acc[pl.ds(at, self.half)] = mine.astype(jnp.bfloat16)
        self.waits = []
        for step in range(1, s.plane):
            to, device = self.plane_device(step)
            src = self.acc.at[pl.ds(at + to * self.part, self.part)]
            dst = self.land_plane.at[step - 1, pl.ds(at // s.plane, self.part)]
            self.waits.append(self.copy(src, dst, device))

    def start_wa(self):
        s = self.s
        for made in self.waits:
            made.wait_recv()
        at = self.base // s.cores
        low = at // s.plane
        total = self.acc[pl.ds(at + self.me * self.part, self.part)].astype(jnp.float32)
        for step in range(1, s.plane):
            total = total + self.land_plane[step - 1, pl.ds(low, self.part)].astype(jnp.float32)
        spare = self.land_plane.at[s.plane - 1]
        spare[pl.ds(low, self.part)] = total.astype(jnp.bfloat16)
        self.waits = []
        for step in range(1, s.nw):
            to, device = self.wa_device(step)
            src = spare.at[pl.ds(low + to * self.shard, self.shard)]
            dst = self.land_wa.at[step - 1, pl.ds(low // s.nw, self.shard)]
            self.waits.append(self.copy(src, dst, device))

    def back_wa(self):
        s = self.s
        for made in self.waits:
            made.wait_recv()
        low = self.base // s.cores // s.plane
        spare = self.land_plane.at[s.plane - 1]
        total = spare[pl.ds(low + self.wi * self.shard, self.shard)].astype(jnp.float32)
        for step in range(1, s.nw):
            total = total + self.land_wa[step - 1, pl.ds(low // s.nw, self.shard)].astype(jnp.float32)
        here = self.first + self.core * self.half + self.me * self.part
        mine = self.out.at[pl.ds(here + self.wi * self.shard, self.shard)]
        mine[...] = total.astype(jnp.bfloat16)
        self.waits = [self.copy(mine, mine, self.wa_device(step)[1]) for step in range(1, s.nw)]

    def back_plane(self):
        s = self.s
        for made in self.waits:
            made.wait_recv()
        here = self.first + self.core * self.half + self.me * self.part
        mine = self.out.at[pl.ds(here, self.part)]
        self.waits = [self.copy(mine, mine, self.plane_device(step)[1]) for step in range(1, s.plane)]

    def back_core(self):
        for made in self.waits:
            made.wait_recv()
        self.waits = []
        if self.s.cores == 2:
            mine = self.out.at[pl.ds(self.first + self.core * self.half, self.half)]
            self.waits = [self.copy(mine, mine, self.core_device())]

    def finish(self):
        for made in self.waits:
            made.wait_recv()
        for made in self.open:
            made.wait_send()


def copies_of(sizes):
    return 2 * ((sizes.cores - 1) + (sizes.plane - 1) + (sizes.nw - 1))


STAGES = ("start_core", "start_plane", "start_wa", "back_wa", "back_plane", "back_core", "finish")


def reduce_scratch(sizes, tiles, count):
    half = tiles // sizes.cores
    part = half // sizes.plane
    return [
        pltpu.VMEM((half, TILE, 128), jnp.bfloat16),
        pltpu.VMEM((sizes.plane, part, TILE, 128), jnp.bfloat16),
        pltpu.VMEM((max(sizes.nw - 1, 1), part // sizes.nw, TILE, 128), jnp.bfloat16),
        pltpu.VMEM((half, TILE, 128), jnp.bfloat16),
        pltpu.SemaphoreType.DMA((count * copies_of(sizes),)),
        pltpu.SemaphoreType.DMA((count * copies_of(sizes),)),
    ]


def reduce_partners(sizes, where):
    ti, hi, wi = where
    core = hi % sizes.cores
    me = ti * sizes.rows + hi // sizes.cores
    found = []
    if sizes.cores == 2:
        found.append((ti, hi + 1 - 2 * core, wi))
    for step in range(1, sizes.plane):
        to = lax.rem(me + step, sizes.plane)
        found.append((to // sizes.rows, (to % sizes.rows) * sizes.cores + core, wi))
    for step in range(1, sizes.nw):
        found.append((ti, hi, lax.rem(wi + step, sizes.nw)))
    return found


DIRS = [(dt, dh) for dt in (-1, 0, 1) for dh in (-1, 0, 1) if (dt, dh) != (0, 0)]


class Halo:
    def __init__(self, sizes, where, sources, landings, send, recv):
        self.s, self.where = sizes, where
        self.sources, self.landings = sources, landings
        self.frames, self.height = sources[0].shape[0], sources[0].shape[1]
        self.send, self.recv = send, recv

    def exists(self, dt, dh):
        ti, hi = self.where[0] + dt, self.where[1] + dh
        return (ti >= 0) & (ti < self.s.nt) & (hi >= 0) & (hi < self.s.nh)

    def made(self, field, dt, dh):
        def span(step, extent):
            first = {-1: 0, 0: 0, 1: extent - 1}[step]
            land = {-1: extent + 1, 0: 1, 1: 0}[step]
            return first, land, extent if step == 0 else 1

        t0, t1, tn = span(dt, self.frames)
        h0, h1, hn = span(dh, self.height)
        slot = field * len(DIRS) + DIRS.index((dt, dh))
        return pltpu.make_async_remote_copy(
            src_ref=self.sources[field].at[pl.ds(t0, tn), pl.ds(h0, hn)],
            dst_ref=self.landings[field].at[pl.ds(t1, tn), pl.ds(h1, hn)],
            send_sem=self.send.at[slot],
            recv_sem=self.recv.at[slot],
            device_id=(self.where[0] + dt, self.where[1] + dh, self.where[2]),
            device_id_type=MESH,
        )

    def start(self):
        for dt, dh in DIRS:

            @pl.when(self.exists(dt, dh))
            def _():
                for field in range(len(self.sources)):
                    self.made(field, dt, dh).start()

    def zero(self):
        def span(step, extent):
            return {-1: (0, 1), 0: (1, extent), 1: (extent + 1, 1)}[step]

        for dt, dh in DIRS:

            @pl.when(jnp.logical_not(self.exists(dt, dh)))
            def _():
                for landing in self.landings:
                    part = landing.at[pl.ds(*span(dt, self.frames)), pl.ds(*span(dh, self.height))]
                    part[...] = jnp.zeros(part.shape, part.dtype)

    def wait_recv(self):
        for dt, dh in DIRS:

            @pl.when(self.exists(-dt, -dh))
            def _():
                for field in range(len(self.sources)):
                    self.made(field, dt, dh).wait_recv()

    def wait_send(self):
        for dt, dh in DIRS:

            @pl.when(self.exists(dt, dh))
            def _():
                for field in range(len(self.sources)):
                    self.made(field, dt, dh).wait_send()


class Columns:
    def __init__(self, sizes, where, landings, lines, shifted, edge_out, edge_in, wide, send, recv):
        self.s, self.where, self.landings, self.lines = sizes, where, landings, lines
        self.shifted, self.out, self.into, self.wide = shifted, edge_out, edge_in, wide
        self.send, self.recv = send, recv
        self.count = landings[0].shape[0] * landings[0].shape[1]
        self.width = landings[0].shape[2]

    def exists(self, side):
        to = self.where[2] + (1 if side else -1)
        return (to >= 0) & (to < self.s.nw)

    def made(self, side):
        return pltpu.make_async_remote_copy(
            src_ref=self.out.at[side],
            dst_ref=self.into.at[1 - side],
            send_sem=self.send.at[side],
            recv_sem=self.recv.at[1 - side],
            device_id=(self.where[0], self.where[1], self.where[2] + (1 if side else -1)),
            device_id_type=MESH,
        )

    def start(self):
        cells = self.count * self.width
        for field, landing in enumerate(self.landings):
            line = self.lines[field]
            line[pl.ds(8, cells), :] = landing[...].astype(jnp.float32).reshape(cells, 128)
            for side in range(2):
                edge = line[pl.ds(8 + side * (self.width - 1), self.count, stride=self.width), :]
                self.out[side, field] = edge.astype(jnp.bfloat16)
        for side in range(2):
            pl.when(self.exists(side))(lambda side=side: self.made(side).start())
            zero = jnp.zeros(self.into.shape[1:], jnp.bfloat16)

            @pl.when(jnp.logical_not(self.exists(side)))
            def _():
                self.into[side] = zero

        frames = self.landings[0].shape[0]
        for field, landing in enumerate(self.landings):
            self.wide[field, :, :, 128:256] = landing[...].reshape(frames, -1, 128)

    def finish(self):
        for side in range(2):
            pl.when(self.exists(side))(lambda side=side: self.made(1 - side).wait_recv())
        cells = self.count * self.width
        frames = self.landings[0].shape[0]
        for field in range(len(self.landings)):
            for side in range(2):
                line = self.lines[field]
                self.shifted[...] = line[pl.ds(7 + 2 * side, cells), :]
                at = side * (self.width - 1)
                edge = self.into[side, field].astype(jnp.float32)
                self.shifted[pl.ds(at, self.count, stride=self.width), :] = edge
                moved = self.shifted[...].astype(jnp.bfloat16).reshape(frames, -1, 128)
                self.wide[field, :, :, 256 * side : 256 * side + 128] = moved

    def wait_send(self):
        for side in range(2):
            pl.when(self.exists(side))(lambda side=side: self.made(side).wait_send())


def conv_rows(wide, field, frame, first, rows, width, weights):
    total = None
    for tap in range(9):
        at = (tap % 3) * width + first
        piece = wide[field, frame + tap // 3, pl.ds(at, rows), :]
        product = jnp.dot(piece, weights[tap], preferred_element_type=jnp.float32)
        total = product if total is None else total + product
    return total


def kernel(
    sizes, ranges, volume, cotangent, one, two, d_volume, sums,
    fields, d_fields, lines, shifted, edge_out, edge_in, d_out, d_in, wide, d_wide,
    flip_one, flip_two, d_pre, part, turned, halo_send, halo_recv, col_send, col_recv, *scratch,
):
    bufs, (send, recv) = scratch[:4], scratch[4:]
    where = (lax.axis_index("ta"), lax.axis_index("ha"), lax.axis_index("wa"))
    frames, height, width, _ = volume.shape
    cells = height * width
    block = 256 if cells % 256 == 0 else cells
    partners = reduce_partners(sizes, where)
    halo = Halo(
        sizes, where, [volume, cotangent], [fields.at[0], fields.at[1]], halo_send.at[0], halo_recv.at[0]
    )
    d_halo = Halo(sizes, where, [d_pre], [d_fields], halo_send.at[1], halo_recv.at[1])
    barrier = pltpu.get_barrier_semaphore()
    for device in partners:
        pl.semaphore_signal(barrier, inc=1, device_id=device, device_id_type=MESH)
    for dt, dh in DIRS:

        @pl.when(halo.exists(dt, dh))
        def _():
            device = (where[0] + dt, where[1] + dh, where[2])
            pl.semaphore_signal(barrier, inc=1, device_id=device, device_id_type=MESH)

    near = sum(halo.exists(dt, dh).astype(jnp.int32) for dt, dh in DIRS)
    pl.semaphore_wait(barrier, len(partners) + near)
    halo.start()
    halo.zero()
    d_halo.zero()
    inner = (pl.ds(1, frames), pl.ds(1, height))
    for field, ref in enumerate((volume, cotangent)):
        fields.at[field].at[inner][...] = ref[...]
    for source, flipped in ((two, flip_two), (one, flip_one)):
        for tap in range(9):
            for kw in range(3):
                square = source[8 - tap, pl.ds((2 - kw) * 128, 128), :].astype(jnp.float32)
                flipped[tap, pl.ds(kw * 128, 128), :] = square.T.astype(jnp.bfloat16)
    halo.wait_recv()
    columns = Columns(
        sizes, where, [fields.at[0], fields.at[1]], [lines.at[0], lines.at[1]], shifted,
        edge_out, edge_in, wide, col_send.at[0], col_recv.at[0],
    )
    columns.start()
    columns.finish()
    for frame in range(frames):
        for first in range(0, cells, block):
            pre = conv_rows(wide, 0, frame, first, block, width, one)
            d_hidden = conv_rows(wide, 1, frame, first, block, width, flip_two)
            sig = 1.0 / (1.0 + jnp.exp(-pre))
            hidden = pre * sig
            grad = d_hidden * sig * (1.0 + pre * (1.0 - sig))
            at = pl.ds(frame * cells + first, block)
            turned[0, :, at] = hidden.T.astype(jnp.bfloat16)
            turned[1, :, at] = grad.T.astype(jnp.bfloat16)
            rounded = grad.astype(jnp.bfloat16).reshape(1, block // width, width, 128)
            d_pre[pl.ds(frame, 1), pl.ds(first // width, block // width)] = rounded
    d_halo.start()
    d_fields.at[inner][...] = d_pre[...]
    middle = part.shape[0] // 2
    real = 27 * 128 // TILE
    for base in (0, middle):
        if middle > real:
            part[pl.ds(base + real, middle - real)] = jnp.zeros((middle - real, TILE, 128), jnp.bfloat16)

    def gradient(field, side, tap):
        total = None
        for frame in range(frames):
            piece = wide[field, frame + tap // 3, pl.ds((tap % 3) * width, cells), :]
            left = turned[side, :, pl.ds(frame * cells, cells)]
            product = jnp.dot(left, piece, preferred_element_type=jnp.float32)
            total = product if total is None else total + product
        return total

    runs = [
        Reduce(sizes, where, part, sums, first, tiles, first, bufs, send, recv, i * copies_of(sizes))
        for i, (first, tiles) in enumerate(ranges)
    ]
    early, late = runs[: len(runs) // 2], runs[len(runs) // 2 :]

    def begin(group, base, tap):
        done = middle if tap == 8 else (tap + 1) * 3 * (128 // TILE)
        while group and group[0].first + group[0].tiles - base <= done:
            group.pop(0).start_core()

    waiting = list(early)
    for tap in range(9):
        product = gradient(1, 0, 8 - tap).astype(jnp.bfloat16)
        for kw in range(3):
            at = (tap * 3 + 2 - kw) * (128 // TILE)
            square = product[:, kw * 128 : kw * 128 + 128]
            part[pl.ds(at, 128 // TILE)] = square.reshape(128 // TILE, TILE, 128)
        begin(waiting, 0, tap)
    waiting, plane = list(late), list(early)
    for tap in range(9):
        product = gradient(0, 1, tap)
        for kw in range(3):
            at = middle + (tap * 3 + kw) * (128 // TILE)
            square = product[:, kw * 128 : kw * 128 + 128].T.astype(jnp.bfloat16)
            part[pl.ds(at, 128 // TILE)] = square.reshape(128 // TILE, TILE, 128)
        begin(waiting, middle, tap)
        if tap % 3 == 1 and plane:
            plane.pop(0).start_plane()
    for run in plane:
        run.start_plane()
    d_halo.wait_recv()
    d_columns = Columns(
        sizes, where, [d_fields], [lines.at[0]], shifted, d_out, d_in, d_wide, col_send.at[1], col_recv.at[1]
    )
    d_columns.start()
    for run in late:
        run.start_plane()

    def volume_part():
        d_columns.finish()
        for frame in range(frames):
            for first in range(0, cells, block):
                total = conv_rows(d_wide, 0, frame, first, block, width, flip_one)
                total = total.astype(jnp.bfloat16).reshape(1, block // width, width, 128)
                d_volume[pl.ds(frame, 1), pl.ds(first // width, block // width)] = total

    order = STAGES[2:-1]
    for wave in range(len(runs) + len(order) - 1):
        for place, run in enumerate(runs):
            if 0 <= wave - place < len(order):
                getattr(run, order[wave - place])()
        if wave == 0:
            volume_part()
    for run in runs:
        run.finish()
    halo.wait_send()
    d_halo.wait_send()
    columns.wait_send()
    d_columns.wait_send()


def body(sizes, volume, cotangent, kernel_one, kernel_two):
    frames, height, width, chans = volume.shape
    real = 27 * chans // TILE
    ranges = chunks_of(real, sizes.devices, 3)
    middle = sum(tiles for _, tiles in ranges)
    ranges = ranges + [(middle + first, tiles) for first, tiles in ranges]
    tiles = 2 * middle
    tall, high = frames + 2, height + 2
    count = tall * high
    half = jnp.bfloat16
    vmem = pl.BlockSpec(memory_space=pltpu.VMEM)
    d_volume, sums = pl.pallas_call(
        functools.partial(kernel, sizes, ranges),
        out_shape=(
            jax.ShapeDtypeStruct(volume.shape, half),
            jax.ShapeDtypeStruct((tiles, TILE, chans), half),
        ),
        in_specs=[vmem] * 4,
        out_specs=(vmem, vmem),
        scratch_shapes=[
            pltpu.VMEM((2, tall, high, width, chans), half),
            pltpu.VMEM((tall, high, width, chans), half),
            pltpu.VMEM((2, count * width + 16, chans), jnp.float32),
            pltpu.VMEM((count * width, chans), jnp.float32),
            pltpu.VMEM((2, 2, count, chans), half),
            pltpu.VMEM((2, 2, count, chans), half),
            pltpu.VMEM((2, 1, count, chans), half),
            pltpu.VMEM((2, 1, count, chans), half),
            pltpu.VMEM((2, tall, high * width, 3 * chans), half),
            pltpu.VMEM((1, tall, high * width, 3 * chans), half),
            pltpu.VMEM((9, 3 * chans, chans), half),
            pltpu.VMEM((9, 3 * chans, chans), half),
            pltpu.VMEM(volume.shape, half),
            pltpu.VMEM((tiles, TILE, chans), half),
            pltpu.VMEM((2, chans, frames * height * width), half),
            pltpu.SemaphoreType.DMA((2, 2 * len(DIRS))),
            pltpu.SemaphoreType.DMA((2, 2 * len(DIRS))),
            pltpu.SemaphoreType.DMA((2, 2)),
            pltpu.SemaphoreType.DMA((2, 2)),
        ]
        + reduce_scratch(sizes, tiles, len(ranges)),
        compiler_params=pltpu.CompilerParams(
            collective_id=0, has_side_effects=True, vmem_limit_bytes=56 * 1024 * 1024
        ),
    )(volume, cotangent, kernel_one.reshape(9, 3 * chans, chans), kernel_two.reshape(9, 3 * chans, chans))
    scale = 1.0 / jnp.sqrt(jnp.float32(frames * height * width * sizes.devices))

    def scaled(first):
        return sums[first : first + real].reshape(kernel_one.shape).astype(jnp.float32) * scale

    return d_volume, scaled(middle), scaled(0)


def solution(mesh):
    in_specs = (P("ta", "ha", "wa", None), P("ta", "ha", "wa", None), P(), P())
    out_specs = (P("ta", "ha", "wa", None), P(), P())
    return jax.shard_map(
        functools.partial(body, Sizes(mesh)),
        mesh=mesh, in_specs=in_specs, out_specs=out_specs, check_vma=False,
    )
```
